32 devices in a mesh: outer: 2 (over y), inner: 4 (over x, core), heads: 4 (over z).
Axes of the slice: x: 2, y: 2, z: 4, core: 2. Of those that a mesh axis runs over, the one named last changes fastest.
Arguments:
- raw_keys: bfloat16 [8, 4096, 8, 128], P(None, ('outer', 'inner'), 'heads'), may hold values from -6 to 6
- raw_values: bfloat16 [8, 4096, 8, 128], P(None, ('outer', 'inner'), 'heads'), may hold values from -6 to 6
- turn_angle: float32 [4096, 64], replicated, may hold values from -3.140625 to 3.140625
Outputs:
- stored_keys: bfloat16 [8, 4096, 8, 128], P(('outer', 'inner'), None, 'heads')
- stored_values: bfloat16 [8, 4096, 8, 128], P(('outer', 'inner'), None, 'heads')
- page_high: bfloat16 [8, 64, 8, 128], P(('outer', 'inner'), None, 'heads')
- page_low: bfloat16 [8, 64, 8, 128], P(('outer', 'inner'), None, 'heads')
The draws below stay inside these ranges and needn't reach their ends.
All inputs are finite; a program needn't handle non-finite values.
Results may differ from the reference program's by a relative error of at most 0.001.
Values may be sent and summed in bfloat16 or wider, within the bound.
A program may use at most 128 MiB of HBM per device.

```python
import jax
import jax.numpy as jnp

BATCH = 8
LENGTH = 4096
KV_HEADS = 8
HEAD_SIZE = 128
HALF_HEAD = 64
PAGE = 64


def block_levels(own_key, extent, shards, smallest, largest):
    factor_of = 1.0
    for axis_at, parts in shards:
        steps = jax.random.uniform(jax.random.fold_in(jax.random.fold_in(own_key, 6), axis_at), (parts,), jnp.float32, smallest / len(shards), largest / len(shards))
        factor_of = factor_of * jnp.repeat(jnp.exp(steps), extent[axis_at] // parts).reshape((-1,) + (1,) * (len(extent) - 1 - axis_at))
    return factor_of


def scatter_about(own_key, shape, deviation, most, split=(), dtype=jnp.bfloat16):
    array = deviation * jax.random.normal(own_key, shape, jnp.float32)
    if split:
        array = array * block_levels(own_key, shape, split, -0.22, 0.18)
    return jnp.clip(array, -most, most).astype(dtype)


def setup_inputs(seed: int = 0) -> dict:
    key_list = jax.random.split(jax.random.key(seed), 4)
    raw_keys = scatter_about(key_list[0], (BATCH, LENGTH, KV_HEADS, HEAD_SIZE), 1.0, 6.0, ((1, 8), (2, 4)))
    raw_values = scatter_about(key_list[1], (BATCH, LENGTH, KV_HEADS, HEAD_SIZE), 1.0, 6.0, ((1, 8), (2, 4)))
    turn_angle = jnp.clip(jax.random.uniform(key_list[2], (LENGTH, HALF_HEAD), jnp.float32, -3.140625, 3.140625), -3.140625, 3.140625)
    return {"raw_keys": raw_keys, "raw_values": raw_values, "turn_angle": turn_angle}


def turn_pairs(vectors, angle):
    half = vectors.shape[-1] // 2
    cosine, sine = jnp.cos(angle)[None, :, None, :], jnp.sin(angle)[None, :, None, :]
    first, second = vectors[..., :half], vectors[..., half:]
    return jnp.concatenate([first * cosine - second * sine, second * cosine + first * sine], axis=-1)


def prepare_keys(plain_keys, angle):
    wide_keys = plain_keys.astype(jnp.float32)
    return turn_pairs(wide_keys, angle)


def reference(raw_keys, raw_values, turn_angle):
    turned_keys = prepare_keys(raw_keys, turn_angle)
    narrow_keys = turned_keys.astype(jnp.bfloat16)
    page_view = narrow_keys.reshape(BATCH, LENGTH // PAGE, PAGE, KV_HEADS, HEAD_SIZE)
    page_high = jnp.max(page_view, axis=2)
    page_low = jnp.min(page_view, axis=2)
    stored_keys = narrow_keys
    stored_values = raw_values
    return stored_keys, stored_values, page_high, page_low
```

```python
import functools

import jax
import jax.numpy as jnp
from jax import lax
from jax.experimental import pallas as pl
from jax.experimental.pallas import tpu as pltpu
from jax.sharding import PartitionSpec as P

PAGE = 64
MESH = pl.DeviceIdType.MESH


def offsets(outer, inner):
    cores = 2 if inner % 2 == 0 else 1
    chips = inner // cores
    steps = [
        (do, dx, dc)
        for dc in range(cores)
        for do in range(outer)
        for dx in range(chips)
        if (do, dx, dc) != (0, 0, 0)
    ]
    return cores, chips, sorted(steps, key=lambda s: (s[0] != 0) + (s[1] != 0))


def kernel(
    outer, inner, heads,
    keys, values, angle,
    out_keys, out_values, out_high, out_low,
    landed, angles, table, wide, turned, bound,
    send_k, recv_k, send_v, recv_v, local,
):
    group = outer * inner
    batch, rows, size = keys.shape
    own = batch // group
    length = rows // heads
    half = size // 2
    pages = length // PAGE
    cores, chips, steps = offsets(outer, inner)
    o, i = lax.axis_index("outer"), lax.axis_index("inner")
    x, c = i // cores, i % cores
    me = o * inner + i

    def partner(step, sign):
        do, dx, dc = step
        po = (o + sign * do + outer) % outer
        pi = (x + sign * dx + chips) % chips * cores + (c + sign * dc + cores) % cores
        return po, pi

    get_angles = pltpu.make_async_copy(angle, angles, local.at[0])
    get_angles.start()
    mine = pl.ds(pl.multiple_of(me * rows, rows), rows)
    own_keys = pltpu.make_async_copy(
        keys.at[pl.ds(me * own, own)], landed.at[:, mine], local.at[1]
    )
    own_values = pltpu.make_async_copy(
        values.at[pl.ds(me * own, own)], out_values.at[:, mine], local.at[2]
    )
    own_keys.start()
    own_values.start()

    barrier = pltpu.get_barrier_semaphore()
    for step in steps:
        po, pi = partner(step, 1)
        pl.semaphore_signal(
            barrier, inc=1, device_id={"outer": po, "inner": pi}, device_id_type=MESH
        )
    pl.semaphore_wait(barrier, len(steps))

    copies_k, copies_v = [], []
    for j, step in enumerate(steps):
        po, pi = partner(step, 1)
        theirs = pl.ds((po * inner + pi) * own, own)
        for copies, src, dst, send, recv in (
            (copies_k, keys, landed, send_k, recv_k),
            (copies_v, values, out_values, send_v, recv_v),
        ):
            copies.append(
                pltpu.make_async_remote_copy(
                    src_ref=src.at[theirs],
                    dst_ref=dst.at[:, mine],
                    send_sem=send.at[j],
                    recv_sem=recv.at[j],
                    device_id={"outer": po, "inner": pi},
                    device_id_type=MESH,
                )
            )
    far = [(s[0] != 0) + (s[1] != 0) for s in steps]
    for distance in sorted(set(far)):
        for copies in (copies_k, copies_v):
            for j, copy in enumerate(copies):
                if far[j] == distance:
                    copy.start()

    get_angles.wait()

    def fill(p, carry):
        at = pl.ds(pl.multiple_of(p * size, size), size)
        a = angles[:, at]
        table[at] = jnp.concatenate([jnp.cos(a), jnp.sin(a)], axis=0).T
        return carry

    lax.fori_loop(0, table.shape[0] // size, fill, 0)

    def turn(source):
        for n in range(own):
            def page(p, carry):
                at = pl.multiple_of(source * length + p * PAGE, PAGE)
                tab = table[pl.ds(at, PAGE)]
                swap = pltpu.roll(tab, half, 1)
                low_half = lax.broadcasted_iota(jnp.int32, tab.shape, 1) < half
                cosine = jnp.where(low_half, tab, swap)
                sine = jnp.where(low_half, -swap, tab)
                at_rows = pl.ds(pl.multiple_of(at * heads, PAGE * heads), PAGE * heads)
                wide[...] = landed[n, at_rows].astype(jnp.float32)
                for h in range(heads):
                    v = wide[pl.ds(h, PAGE, stride=heads)]
                    y = v * cosine + pltpu.roll(v, half, 1) * sine
                    turned[pl.ds(h, PAGE, stride=heads)] = y
                    bound[0, pl.ds(p * heads + h, 1)] = jnp.max(y, axis=0, keepdims=True)
                    bound[1, pl.ds(p * heads + h, 1)] = jnp.min(y, axis=0, keepdims=True)
                out_keys[n, at_rows] = turned[...].astype(out_keys.dtype)
                return carry

            lax.fori_loop(0, pages, page, 0)
            at_pages = pl.ds(pl.multiple_of(source * pages * heads, pages * heads), pages * heads)
            out_high[n, at_pages] = bound[0].astype(out_high.dtype)
            out_low[n, at_pages] = bound[1].astype(out_low.dtype)

    own_keys.wait()
    turn(me)
    for j, step in enumerate(steps):
        copies_k[j].wait_recv()
        po, pi = partner(step, -1)
        turn(po * inner + pi)
    own_values.wait()
    for j in range(len(steps)):
        copies_v[j].wait_recv()
    for j in range(len(steps)):
        copies_k[j].wait_send()
        copies_v[j].wait_send()


def per_device(outer, inner, raw_keys, raw_values, turn_angle):
    batch, length, heads, size = raw_keys.shape
    group = outer * inner
    own, rows, pages = batch // group, length * heads, length // PAGE
    bf16, f32 = jnp.bfloat16, jnp.float32
    scratch_bytes = group * length * size * (2 * own * heads + 8) + 2**22
    outs = pl.pallas_call(
        functools.partial(kernel, outer, inner, heads),
        out_shape=(
            pltpu.VMEM((own, group * rows, size), bf16),
            pltpu.VMEM((own, group * rows, size), bf16),
            pltpu.VMEM((own, group * pages * heads, size), bf16),
            pltpu.VMEM((own, group * pages * heads, size), bf16),
        ),
        in_specs=[pl.BlockSpec(memory_space=pltpu.HBM)] * 3,
        out_specs=[pl.BlockSpec(memory_space=pltpu.VMEM)] * 4,
        scratch_shapes=[
            pltpu.VMEM((own, group * rows, size), bf16),
            pltpu.VMEM((turn_angle.shape[1], turn_angle.shape[0]), f32),
            pltpu.VMEM((turn_angle.shape[0], size), f32),
            pltpu.VMEM((PAGE * heads, size), f32),
            pltpu.VMEM((PAGE * heads, size), f32),
            pltpu.VMEM((2, pages * heads, size), f32),
            pltpu.SemaphoreType.DMA((group,)),
            pltpu.SemaphoreType.DMA((group,)),
            pltpu.SemaphoreType.DMA((group,)),
            pltpu.SemaphoreType.DMA((group,)),
            pltpu.SemaphoreType.DMA((3,)),
        ],
        compiler_params=pltpu.CompilerParams(
            collective_id=0, has_side_effects=True, vmem_limit_bytes=scratch_bytes
        ),
    )(
        raw_keys.reshape(batch, rows, size),
        raw_values.reshape(batch, rows, size),
        turn_angle.T,
    )
    keys, values, high, low = outs
    return (
        keys.reshape(own, group * length, heads, size),
        values.reshape(own, group * length, heads, size),
        high.reshape(own, group * pages, heads, size),
        low.reshape(own, group * pages, heads, size),
    )


def solution(mesh):
    moved = P(None, ("outer", "inner"), "heads", None)
    whole = P(("outer", "inner"), None, "heads", None)
    return jax.shard_map(
        functools.partial(per_device, mesh.shape["outer"], mesh.shape["inner"]),
        mesh=mesh,
        in_specs=(moved, moved, P()),
        out_specs=(whole,) * 4,
        check_vma=False,
    )
```

```python
import functools

import jax
import jax.numpy as jnp
from jax import lax
from jax.experimental import pallas as pl
from jax.experimental.pallas import tpu as pltpu
from jax.sharding import PartitionSpec as P

PAGE = 64
MESH = pl.DeviceIdType.MESH


def offsets(outer, inner):
    cores = 2 if inner % 2 == 0 else 1
    chips = inner // cores
    steps = [
        (do, dx, dc)
        for dc in range(cores)
        for do in range(outer)
        for dx in range(chips)
        if (do, dx, dc) != (0, 0, 0)
    ]
    return cores, chips, sorted(steps, key=lambda s: (s[0] != 0) + (s[1] != 0))


def kernel(
    outer, inner, heads,
    keys, values, angle,
    out_keys, out_values, out_high, out_low,
    landed, angles, table, wide, turned, bound,
    send_k, recv_k, send_v, recv_v, local,
):
    group = outer * inner
    batch, rows, size = keys.shape
    own = batch // group
    length = rows // heads
    half = size // 2
    pages = length // PAGE
    cores, chips, steps = offsets(outer, inner)
    o, i = lax.axis_index("outer"), lax.axis_index("inner")
    x, c = i // cores, i % cores
    me = o * inner + i

    def partner(step, sign):
        do, dx, dc = step
        po = (o + sign * do + outer) % outer
        pi = (x + sign * dx + chips) % chips * cores + (c + sign * dc + cores) % cores
        return po, pi

    get_angles = pltpu.make_async_copy(angle, angles, local.at[0])
    get_angles.start()
    mine = pl.ds(pl.multiple_of(me * rows, rows), rows)
    own_keys = pltpu.make_async_copy(
        keys.at[pl.ds(me * own, own)], landed.at[:, mine], local.at[1]
    )
    own_values = pltpu.make_async_copy(
        values.at[pl.ds(me * own, own)], out_values.at[:, mine], local.at[2]
    )
    own_keys.start()
    own_values.start()

    barrier = pltpu.get_barrier_semaphore()
    for step in steps:
        po, pi = partner(step, 1)
        pl.semaphore_signal(
            barrier, inc=1, device_id={"outer": po, "inner": pi}, device_id_type=MESH
        )
    pl.semaphore_wait(barrier, len(steps))

    copies_k, copies_v = [], []
    for j, step in enumerate(steps):
        po, pi = partner(step, 1)
        theirs = pl.ds((po * inner + pi) * own, own)
        for copies, src, dst, send, recv in (
            (copies_k, keys, landed, send_k, recv_k),
            (copies_v, values, out_values, send_v, recv_v),
        ):
            copies.append(
                pltpu.make_async_remote_copy(
                    src_ref=src.at[theirs],
                    dst_ref=dst.at[:, mine],
                    send_sem=send.at[j],
                    recv_sem=recv.at[j],
                    device_id={"outer": po, "inner": pi},
                    device_id_type=MESH,
                )
            )
    far = [(s[0] != 0) + (s[1] != 0) for s in steps]
    for distance in sorted(set(far)):
        for copies in (copies_k, copies_v):
            for j, copy in enumerate(copies):
                if far[j] == distance:
                    copy.start()

    get_angles.wait()

    def fill(p, carry):
        at = pl.ds(pl.multiple_of(p * size, size), size)
        a = angles[:, at]
        table[at] = jnp.concatenate([jnp.cos(a), jnp.sin(a)], axis=0).T
        return carry

    lax.fori_loop(0, table.shape[0] // size, fill, 0)

    def turn(source):
        for n in range(own):
            def page(p, carry):
                at = pl.multiple_of(source * length + p * PAGE, PAGE)
                tab = table[pl.ds(at, PAGE)]
                swap = pltpu.roll(tab, half, 1)
                low_half = lax.broadcasted_iota(jnp.int32, tab.shape, 1) < half
                cosine = jnp.where(low_half, tab, swap)
                sine = jnp.where(low_half, -swap, tab)
                at_rows = pl.ds(pl.multiple_of(at * heads, PAGE * heads), PAGE * heads)
                wide[...] = landed[n, at_rows].astype(jnp.float32)
                for h in range(heads):
                    v = wide[pl.ds(h, PAGE, stride=heads)]
                    y = v * cosine + pltpu.roll(v, half, 1) * sine
                    turned[pl.ds(h, PAGE, stride=heads)] = y
                    bound[0, pl.ds(p * heads + h, 1)] = jnp.max(y, axis=0, keepdims=True)
                    bound[1, pl.ds(p * heads + h, 1)] = jnp.min(y, axis=0, keepdims=True)
                out_keys[n, at_rows] = turned[...].astype(out_keys.dtype)
                return carry

            lax.fori_loop(0, pages, page, 0)
            at_pages = pl.ds(pl.multiple_of(source * pages * heads, pages * heads), pages * heads)
            out_high[n, at_pages] = bound[0].astype(out_high.dtype)
            out_low[n, at_pages] = bound[1].astype(out_low.dtype)

    own_keys.wait()
    turn(me)
    for j, step in enumerate(steps):
        copies_k[j].wait_recv()
        po, pi = partner(step, -1)
        turn(po * inner + pi)
    own_values.wait()
    for j in range(len(steps)):
        copies_v[j].wait_recv()
    for j in range(len(steps)):
        copies_k[j].wait_send()
        copies_v[j].wait_send()


def in_hbm(array):
    return pltpu.with_memory_space_constraint(array, pltpu.HBM)


def store(*refs):
    count = len(refs) // 2
    sems = refs[-1]
    copies = [
        pltpu.make_async_copy(refs[k], refs[count + k], sems.at[k]) for k in range(count)
    ]
    for copy in copies:
        copy.start()
    for copy in copies:
        copy.wait()


def per_device(outer, inner, raw_keys, raw_values, turn_angle):
    batch, length, heads, size = raw_keys.shape
    group = outer * inner
    own, rows, pages = batch // group, length * heads, length // PAGE
    bf16, f32 = jnp.bfloat16, jnp.float32
    scratch_bytes = group * length * size * (2 * own * heads + 8) + 2**22
    outs = pl.pallas_call(
        functools.partial(kernel, outer, inner, heads),
        out_shape=(
            pltpu.VMEM((own, group * rows, size), bf16),
            pltpu.VMEM((own, group * rows, size), bf16),
            pltpu.VMEM((own, group * pages * heads, size), bf16),
            pltpu.VMEM((own, group * pages * heads, size), bf16),
        ),
        in_specs=[pl.BlockSpec(memory_space=pltpu.HBM)] * 3,
        out_specs=[pl.BlockSpec(memory_space=pltpu.VMEM)] * 4,
        scratch_shapes=[
            pltpu.VMEM((own, group * rows, size), bf16),
            pltpu.VMEM((turn_angle.shape[1], turn_angle.shape[0]), f32),
            pltpu.VMEM((turn_angle.shape[0], size), f32),
            pltpu.VMEM((PAGE * heads, size), f32),
            pltpu.VMEM((PAGE * heads, size), f32),
            pltpu.VMEM((2, pages * heads, size), f32),
            pltpu.SemaphoreType.DMA((group,)),
            pltpu.SemaphoreType.DMA((group,)),
            pltpu.SemaphoreType.DMA((group,)),
            pltpu.SemaphoreType.DMA((group,)),
            pltpu.SemaphoreType.DMA((3,)),
        ],
        compiler_params=pltpu.CompilerParams(
            collective_id=0, has_side_effects=True, vmem_limit_bytes=scratch_bytes
        ),
    )(
        in_hbm(raw_keys.reshape(batch, rows, size)),
        in_hbm(raw_values.reshape(batch, rows, size)),
        in_hbm(turn_angle.T),
    )
    keys, values, high, low = pl.pallas_call(
        store,
        out_shape=[jax.ShapeDtypeStruct(out.shape, out.dtype) for out in outs],
        in_specs=[pl.BlockSpec(memory_space=pltpu.VMEM)] * 4,
        out_specs=[pl.BlockSpec(memory_space=pltpu.HBM)] * 4,
        scratch_shapes=[pltpu.SemaphoreType.DMA((4,))],
        compiler_params=pltpu.CompilerParams(vmem_limit_bytes=2**20),
    )(*outs)
    return (
        keys.reshape(own, group * length, heads, size),
        values.reshape(own, group * length, heads, size),
        high.reshape(own, group * pages, heads, size),
        low.reshape(own, group * pages, heads, size),
    )


def solution(mesh):
    moved = P(None, ("outer", "inner"), "heads", None)
    whole = P(("outer", "inner"), None, "heads", None)
    return jax.shard_map(
        functools.partial(per_device, mesh.shape["outer"], mesh.shape["inner"]),
        mesh=mesh,
        in_specs=(moved, moved, P()),
        out_specs=(whole,) * 4,
        check_vma=False,
    )
```
